32 devices in a mesh: ice: 4 (over x, core), ocn: 8 (over z, y).
Axes of the slice: x: 2, y: 2, z: 4, core: 2. Of those that a mesh axis runs over, the one named last changes fastest.
Arguments:
- ice_state: bfloat16 [5, 20, 32768], P(None, None, ('ice', 'ocn')), may hold values from -6 to 6
- ocean_state: bfloat16 [5, 20, 32768], P(None, None, ('ice', 'ocn')), may hold values from -5 to 5
- ice_rate: float32 [5, 20], replicated, may hold values from 0.2 to 2
- block_weights: bfloat16 [1024, 128, 128], P(('ice', 'ocn')), may hold values from -0.375 to 0.375
- block_route: int32 [1024, 1], P(('ice', 'ocn')), may hold values from 0 to 31; in each aligned block of 32 rows (0 to 31, 32 to 63, ...) at most 2 rows name the same one
- block_tiles: int32 [1024, 2], P(('ice', 'ocn')), may hold values from 0 to 7
- block_valid: int32 [1024], P(('ice', 'ocn')), may hold values from 16 to 128
- ice_mask: int32 [32768], P(('ice', 'ocn')), may hold values 0 or 1
Outputs:
- ice_final: bfloat16 [5, 20, 32768], P(None, None, ('ice', 'ocn'))
- ocean_flux: bfloat16 [5, 20, 32768], P(None, None, ('ice', 'ocn'))
The draws below stay inside these ranges and needn't reach their ends.
Inputs may be any that keep to these rules, and one draw needn't show every extreme that they name: `block_route`: among the blocks of one device no destination appears more than 2 times.
All inputs are finite; a program needn't handle non-finite values. No bound on the sum of `ice_mask` on one device may be relied on, other than what follows from the above.
Results may differ from the reference program's by a relative error of at most 0.008.
Values may be sent and summed in bfloat16 or wider, within the bound.
A program may use at most 128 MiB of HBM per device.

```python
import math
import jax
import jax.numpy as jnp
import numpy as np
from jax import lax

CATS = 5
FIELDS = 20
BLOCK = 128
CAP = 2
TILES = 8
NB = 32
NI = 32768
NO = 32768
DEVICES = 32


def with_ends(values, stream_key, low, top_value):
    place = [jax.random.randint(jax.random.fold_in(stream_key, axis), (), 0, length) for axis, length in enumerate(values.shape)]
    widest = values.shape.index(max(values.shape))
    next_to = place[:widest] + [(place[widest] + 1) % values.shape[widest]] + place[widest + 1:]
    return values.at[tuple(place)].set(low).at[tuple(next_to)].set(top_value)


def levels(rng, extent, pieces, low, high):
    def one(position, shards_of):
        draws = jax.random.uniform(jax.random.fold_in(jax.random.fold_in(rng, 6), position), (shards_of,), jnp.float32, low / len(pieces), high / len(pieces))
        return jnp.repeat(jnp.exp(draws), extent[position] // shards_of).reshape((-1,) + (1,) * (len(extent) - position - 1))

    gain = one(*pieces[0])
    for cut in pieces[1:]:
        gain = gain * one(*cut)
    return gain


def routed_block(own_key, own, number, rows, count, top, reach, slope):
    ranking = jax.random.permutation(own_key, count)
    packed, ordinary = shares(count, rows * top, reach, slope, True), shares(count, rows * top, reach, slope, False)
    places = jnp.arange(count)

    def named(lengths, turn):
        used = int((lengths > 0).sum())
        fixed = max(1, used // 4)
        shifted = fixed + (places - fixed + turn * (used - fixed)) % max(1, count - fixed)
        return jnp.zeros((count,), jnp.int32).at[ranking[jnp.where(places < fixed, places, shifted)]].set(jnp.asarray(lengths, jnp.int32))

    lengths = jnp.where(number % 4 == 0, named(packed, number // 4), named(ordinary, number - number // 4 - 1))
    mixed = jax.random.permutation(jax.random.fold_in(own, 3), count)
    donor, receiver = mixed[0:count // 2 * 2:2], mixed[1:count // 2 * 2:2]
    slack = jnp.minimum(lengths[donor] - 1, reach - lengths[receiver]) // 2
    slack = jnp.where((donor == ranking[0]) | (receiver == ranking[0]) | (lengths[receiver] == 0), 0, jnp.maximum(slack, 0))
    shifted = jax.random.randint(jax.random.fold_in(own, 4), (count // 2,), 0, 1 << 20) % (slack + 1)
    lengths = lengths.at[donor].add(-shifted).at[receiver].add(shifted)
    members = jnp.searchsorted(jnp.cumsum(lengths), jnp.arange(rows * top), side="right").astype(jnp.int32)
    listing = members.reshape(top, rows).T
    listing = listing[jax.random.permutation(jax.random.fold_in(own, 1), rows)]
    turn = jax.random.randint(jax.random.fold_in(own, 2), (rows, 1), 0, top)
    return jnp.take_along_axis(listing, (jnp.arange(top)[None, :] + turn) % top, axis=1)


def shares(amount, total, limit, slope, full):
    weights = [(1 << 20) // math.isqrt(standing ** slope) + 1 for standing in range(1, amount + 1)]
    largest = limit if full else min(limit, max(-(-total // amount), total * weights[0] // sum(weights)))
    least = 1 if total - largest >= amount - 1 else 0
    holding, rest = [largest] + [least] * (amount - 1), total - largest - least * (amount - 1)
    while rest > 0:
        free = [i for i in range(1, amount) if holding[i] < largest] or [i for i in range(1, amount) if holding[i] < limit]
        whole, left = sum([weights[i] for i in free]), rest
        for i in free:
            addition = min(limit - holding[i], max(1, left * weights[i] // whole), rest)
            holding[i] = holding[i] + addition
            rest = rest - addition
    return np.array(holding)


def normal_values(own_key, shape, deviation, reach, pieces=(), held_as=jnp.bfloat16):
    array = deviation * jax.random.normal(own_key, shape, jnp.float32)
    if pieces:
        array = array * levels(own_key, shape, pieces, -0.22, 0.18)
    return jnp.clip(array, -reach, reach).astype(held_as)


def setup_inputs(seed: int = 0) -> dict:
    streams_of = jax.random.split(jax.random.key(seed), 9)
    ice_state = normal_values(streams_of[0], (CATS, FIELDS, NI), 1.0, 6.0, ((2, 32),))
    ocean_state = normal_values(streams_of[1], (CATS, FIELDS, NO), 0.7, 5.0, ((2, 32),))
    ice_rate = jnp.clip(jnp.exp(jax.random.uniform(streams_of[2], (CATS, FIELDS), jnp.float32, math.log(0.2), math.log(2.0))), 0.2, 2.0)
    block_weights = normal_values(streams_of[3], (NB * DEVICES, BLOCK, BLOCK), (NB * BLOCK // (2 * TILES)) ** -0.5, 0.375, ((0, 32),))
    block_route_keys = jax.random.split(jax.random.fold_in(streams_of[4], 1), (NB * DEVICES) // NB)
    block_route_turns = jax.random.permutation(jax.random.fold_in(streams_of[4], 3), (NB * DEVICES) // NB)
    block_route = jax.vmap(lambda own, number: routed_block(jax.random.fold_in(streams_of[4], 2), own, number, NB, DEVICES, 1, CAP, 1))(block_route_keys, block_route_turns).reshape((NB * DEVICES, 1))
    block_tiles = with_ends(jax.random.randint(streams_of[5], (NB * DEVICES, 2), 0, TILES), jax.random.fold_in(streams_of[5], 1), 0, TILES - 1).astype(jnp.int32)
    block_valid = with_ends(jax.random.randint(streams_of[6], (NB * DEVICES,), BLOCK // 8, BLOCK + 1), jax.random.fold_in(streams_of[6], 1), BLOCK // 8, BLOCK).astype(jnp.int32)
    ice_mask = with_ends((jax.random.randint(streams_of[7], (NI,), 0, 4) < 3).astype(jnp.int32), jax.random.fold_in(streams_of[7], 1), 0, 1)
    return {"ice_state": ice_state, "ocean_state": ocean_state, "ice_rate": ice_rate, "block_weights": block_weights, "block_route": block_route, "block_tiles": block_tiles, "block_valid": block_valid, "ice_mask": ice_mask}


def reference(ice_state, ocean_state, ice_rate, block_weights, block_route, block_tiles, block_valid, ice_mask):
    chans = CATS * FIELDS
    live = jnp.arange(BLOCK, dtype=jnp.int32)[None, :] < block_valid[:, None]
    masked = jnp.where(live[:, :, None], block_weights, jnp.zeros((), jnp.bfloat16)).reshape(DEVICES, NB, BLOCK, BLOCK)
    route = block_route[:, 0].reshape(DEVICES, NB)
    source = block_tiles[:, 0].reshape(DEVICES, NB)
    target = (route * TILES + block_tiles[:, 1].reshape(DEVICES, NB)).astype(jnp.int32)
    rates = ice_rate.reshape(chans, 1).astype(jnp.float32)
    land = ice_mask.astype(jnp.float32)[None, :]
    ocean = ocean_state.reshape(chans, NO).astype(jnp.float32)
    ice = (ice_state * ice_mask.astype(jnp.bfloat16)[None, None, :]).reshape(chans, NI)
    flux = None
    for turn in range(2):
        tiles_all = jnp.transpose(ice.reshape(chans, DEVICES, TILES, BLOCK), (1, 0, 2, 3))

        def forward(acc, item):
            tile_set, weights, picks, places = item
            picked = tile_set[:, picks, :].astype(jnp.float32)
            prods = jnp.einsum("cbi,bio->bco", picked, weights.astype(jnp.float32)).astype(jnp.bfloat16)
            prods = lax.optimization_barrier(prods).astype(jnp.float32)
            return acc.at[places].add(prods), None

        start = jnp.zeros((DEVICES * TILES, chans, BLOCK), jnp.float32)
        ocean_in, unused = lax.scan(forward, start, (tiles_all, masked, source, target))
        ocean_in = jnp.transpose(ocean_in, (1, 0, 2)).reshape(chans, NO)
        flux = jnp.tanh(ocean_in + ocean).astype(jnp.bfloat16)
        flux_tiles = jnp.transpose(flux.reshape(chans, DEVICES * TILES, BLOCK), (1, 0, 2))

        def backward(carry, item):
            weights, picks, places = item
            taken = flux_tiles[places].astype(jnp.float32)
            contrib = jnp.einsum("bco,bio->bci", taken, weights.astype(jnp.float32))
            forced = jnp.zeros((TILES, chans, BLOCK), jnp.float32).at[picks].add(contrib)
            return carry, forced

        unused, forcing = lax.scan(backward, jnp.float32(0.0), (masked, source, target))
        forcing = jnp.transpose(forcing, (2, 0, 1, 3)).reshape(chans, NI)
        ice = (land * (ice.astype(jnp.float32) + rates * jnp.tanh(forcing))).astype(jnp.bfloat16)
    return ice.reshape(CATS, FIELDS, NI), flux.reshape(CATS, FIELDS, NO)
```

```python
import functools

import jax
import jax.numpy as jnp
from jax import lax
from jax.experimental import pallas as pl
from jax.experimental.pallas import tpu as pltpu
from jax.sharding import PartitionSpec as P

CAP = 2
AXES = ("ice", "ocn")
LINE = 4
ROWS = 16


def spread(first, count):
    return sorted(range(first, count), key=lambda c: min(c, count - c))


def kernel(
    sizes, blk_ref, tile_ref, meta_ref, ohf_ref, ohb_ref,
    ice_in, ocean_ref, rate_ref, land_ref, w_ref,
    ice_ref, flux_out,
    psend, prec, zsend, zrec, frec, bsend, ret, contrib, total,
    ps_s, ps_r, zs_s, zs_r, fs_s, fs_r, bs_s, bs_r,
):
    Z, Y, N, tiles = sizes
    chans, width = ice_in.shape[1:]
    per = N * CAP
    steps = chans // ROWS
    ice_id, ocn_id = lax.axis_index("ice"), lax.axis_index("ocn")
    z, y = ocn_id // Y, ocn_id % Y
    p = ice_id * Y + y

    def plane(j):
        q = (p + j) % N
        return {"ice": q // Y, "ocn": z * Y + q % Y}

    def line(c):
        return {"ice": ice_id, "ocn": ((z + c) % Z) * Y + y}

    barrier = pltpu.get_barrier_semaphore()
    for j in range(1, N):
        pl.semaphore_signal(barrier, inc=1, device_id=plane(j), device_id_type=pl.DeviceIdType.MESH)
    for c in range(1, Z):
        pl.semaphore_signal(barrier, inc=1, device_id=line(c), device_id_type=pl.DeviceIdType.MESH)
    pl.semaphore_wait(barrier, N - 1 + Z - 1)

    def remote(src, dst, s, r, dev):
        return pltpu.make_async_remote_copy(
            src_ref=src, dst_ref=dst, send_sem=s, recv_sem=r,
            device_id=dev, device_id_type=pl.DeviceIdType.MESH,
        )

    def pcopy(c, j):
        at = pl.ds((c * N + j) * CAP, CAP)
        return remote(psend.at[at], prec.at[at], ps_s.at[c, j], ps_r.at[c, j], plane(j))

    def bcopy(c, j):
        at = pl.ds((c * N + j) * CAP, CAP)
        return remote(bsend.at[at], ret.at[at], bs_s.at[c, j], bs_r.at[c, j], plane(N - j))

    def zcopy(c):
        return remote(zsend.at[c], zrec.at[c], zs_s.at[c], zs_r.at[c], line(c))

    def fcopy(c):
        return remote(frec[0], frec[c], fs_s.at[c], fs_r.at[c], line(c))

    def gather(load, weights, base, start, finish):
        def rows(r, carry):
            at = pl.ds(pl.multiple_of(r * ROWS, ROWS), ROWS)

            def add(k, accs):
                x = load(k, at)
                return tuple(
                    accs[t] + weights[(base + k) * tiles + t] * x for t in range(tiles)
                )

            accs = lax.fori_loop(0, per, add, tuple(start(t, at) for t in range(tiles)), unroll=True)
            for t in range(tiles):
                finish(t, at, accs[t])
            return carry

        lax.fori_loop(0, steps, rows, 0)

    ice_ref[...] = ice_in[...]
    near = spread(1, Z)

    def turn(number, carry):
        for c in near[::-1] + [0]:
            for n in range(per):
                slot = c * per + n
                block = blk_ref[slot]
                prod = jnp.dot(
                    ice_ref[tile_ref[slot]], w_ref[block], preferred_element_type=jnp.float32
                ).astype(jnp.bfloat16)
                if n < CAP:
                    prec[slot] = prod
                else:
                    psend[slot] = prod
            for j in range(1, N):
                pcopy(c, j).start()
        for c in near[::-1] + [0]:
            for j in range(1, N):
                pcopy(c, j).wait_recv()
            base = c * per

            def load(k, at):
                return prec[base + k, at, :].astype(jnp.float32)

            def start(t, at):
                return jnp.zeros((ROWS, width), jnp.float32)

            def finish(t, at, acc):
                if c == 0:
                    total[t, at, :] = acc
                else:
                    zsend[c, t, at, :] = acc.astype(jnp.bfloat16)

            gather(load, ohf_ref, base, start, finish)
            if c:
                zcopy(c).start()
        for c in near:
            zcopy(c).wait_recv()

        def flux_rows(r, carry):
            at = pl.ds(pl.multiple_of(r * ROWS, ROWS), ROWS)
            for t in range(tiles):
                acc = total[t, at, :]
                for c in near:
                    acc = acc + zrec[c, t, at, :].astype(jnp.float32)
                acc = jnp.tanh(acc + ocean_ref[t, at, :].astype(jnp.float32))
                frec[0][t, at, :] = acc.astype(jnp.bfloat16)
                total[t, at, :] = jnp.zeros((ROWS, width), jnp.float32)
            return carry

        lax.fori_loop(0, steps, flux_rows, 0)
        for c in near:
            fcopy(c).start()
        for c in [0] + near:
            held = (Z - c) % Z
            if c:
                fcopy(held).wait_recv()
            for n in range(per):
                slot = c * per + n
                tile = frec[held][meta_ref[slot]]
                if n < CAP:
                    ret[slot] = tile
                else:
                    bsend[slot] = tile
            for j in range(1, N):
                bcopy(c, j).start()
        for c in [0] + near:
            for j in range(1, N):
                bcopy(c, j).wait_recv()
            base = c * per
            for n in range(per):
                contrib[n] = lax.dot_general(
                    ret[base + n], w_ref[blk_ref[base + n]], (((1,), (1,)), ((), ())),
                    preferred_element_type=jnp.float32,
                )

            def load(k, at):
                return contrib[k, at, :]

            def start(t, at):
                return total[t, at, :]

            def finish(t, at, acc):
                total[t, at, :] = acc

            gather(load, ohb_ref, base, start, finish)

        def ice_rows(r, carry):
            at = pl.ds(pl.multiple_of(r * ROWS, ROWS), ROWS)
            rate = rate_ref[at, :]
            for t in range(tiles):
                old = ice_ref[t, at, :].astype(jnp.float32)
                new = land_ref[pl.ds(t, 1), :] * (old + rate * jnp.tanh(total[t, at, :]))
                ice_ref[t, at, :] = new.astype(jnp.bfloat16)
            return carry

        lax.fori_loop(0, steps, ice_rows, 0)
        for c in range(Z):
            for j in range(1, N):
                pcopy(c, j).wait_send()
                bcopy(c, j).wait_send()
        for c in near:
            zcopy(c).wait_send()
            fcopy(c).wait_send()
        return carry

    lax.fori_loop(0, 2, turn, 0)
    flux_out[...] = frec[0][...]


def on_device(
    ice_state, ocean_state, ice_rate, block_weights, block_route, block_tiles, block_valid, ice_mask
):
    cats, fields, cells = ice_state.shape
    chans = cats * fields
    rows = -(-chans // ROWS) * ROWS
    blocks, width, unused = block_weights.shape
    tiles = cells // width
    outer = lax.axis_size("ocn")
    Z = LINE if outer % LINE == 0 else outer
    Y = outer // Z
    N = lax.axis_size("ice") * Y
    ice_id, ocn_id = lax.axis_index("ice"), lax.axis_index("ocn")
    z, y = ocn_id // Y, ocn_id % Y
    p = ice_id * Y + y

    def number(q, zz):
        return ((q // Y) * outer + zz * Y + q % Y).astype(jnp.int32)

    route = block_route[:, 0]
    source, target = block_tiles[:, 0], block_tiles[:, 1]
    order = jnp.arange(blocks, dtype=jnp.int32)
    earlier = (route[None, :] == route[:, None]) & (order[None, :] < order[:, None])
    slot = jnp.sum(earlier.astype(jnp.int32), axis=1)
    gathered = lax.all_gather((route * tiles + target) * CAP + slot, AXES, axis=0, tiled=False)
    gathered = gathered.reshape(-1, blocks)

    js = jnp.arange(N, dtype=jnp.int32)
    cs = jnp.arange(Z, dtype=jnp.int32)
    ks = jnp.arange(CAP, dtype=jnp.int32)
    ts = jnp.arange(tiles, dtype=jnp.int32)
    dest = number((p + js)[None, :] % N, ((z + cs) % Z)[:, None])
    code = route * CAP + slot
    sel = code == (dest[:, :, None] * CAP + ks)[..., None]
    blk = jnp.sum(jnp.where(sel, order, 0), axis=-1).reshape(-1)
    src = jnp.sum(jnp.where(sel, source, 0), axis=-1).reshape(-1)
    some = jnp.any(sel, axis=-1).reshape(-1)
    ohb = ((src[:, None] == ts) & some[:, None]).astype(jnp.float32).reshape(-1)
    theirs = gathered[number((p - js) % N, z)]
    key = (theirs // (tiles * CAP)) * CAP + theirs % CAP
    own = number(p, (z + cs) % Z)
    rsel = key[None, :, None, :] == (own[:, None] * CAP + ks)[:, None, :, None]
    meta = jnp.sum(jnp.where(rsel, ((theirs // CAP) % tiles)[None, :, None, :], 0), axis=-1).reshape(-1)
    rsome = jnp.any(rsel, axis=-1).reshape(-1)
    ohf = ((meta[:, None] == ts) & rsome[:, None]).astype(jnp.float32).reshape(-1)

    live = jnp.arange(width, dtype=jnp.int32)[None, :] < block_valid[:, None]
    masked = jnp.where(live[:, :, None], block_weights, jnp.zeros((), jnp.bfloat16))

    def tiled(values):
        values = values.reshape(chans, tiles, width).transpose(1, 0, 2)
        return jnp.pad(values, ((0, 0), (0, rows - chans), (0, 0)))

    ice = tiled(ice_state * ice_mask.astype(jnp.bfloat16)[None, None, :])
    ocean = tiled(ocean_state)
    rates = jnp.broadcast_to(jnp.pad(ice_rate.reshape(chans, 1), ((0, rows - chans), (0, 0))), (rows, width))
    land = ice_mask.astype(jnp.float32).reshape(tiles, width)
    slots = Z * N * CAP
    smem, vmem = pl.BlockSpec(memory_space=pltpu.SMEM), pl.BlockSpec(memory_space=pltpu.VMEM)
    tile = (rows, width)
    ice, flux = pl.pallas_call(
        functools.partial(kernel, (Z, Y, N, tiles)),
        out_shape=(jax.ShapeDtypeStruct((tiles,) + tile, jnp.bfloat16),) * 2,
        in_specs=[smem] * 5 + [vmem] * 5,
        out_specs=(vmem, vmem),
        scratch_shapes=[
            pltpu.VMEM((slots,) + tile, jnp.bfloat16),
            pltpu.VMEM((slots,) + tile, jnp.bfloat16),
            pltpu.VMEM((Z, tiles) + tile, jnp.bfloat16),
            pltpu.VMEM((Z, tiles) + tile, jnp.bfloat16),
            tuple(pltpu.VMEM((tiles,) + tile, jnp.bfloat16) for c in range(Z)),
            pltpu.VMEM((slots,) + tile, jnp.bfloat16),
            pltpu.VMEM((slots,) + tile, jnp.bfloat16),
            pltpu.VMEM((N * CAP,) + tile, jnp.float32),
            pltpu.VMEM((tiles,) + tile, jnp.float32),
            pltpu.SemaphoreType.DMA((Z, N)),
            pltpu.SemaphoreType.DMA((Z, N)),
            pltpu.SemaphoreType.DMA((Z,)),
            pltpu.SemaphoreType.DMA((Z,)),
            pltpu.SemaphoreType.DMA((Z,)),
            pltpu.SemaphoreType.DMA((Z,)),
            pltpu.SemaphoreType.DMA((Z, N)),
            pltpu.SemaphoreType.DMA((Z, N)),
        ],
        compiler_params=pltpu.CompilerParams(
            collective_id=0, has_side_effects=True, vmem_limit_bytes=60 * 1024 * 1024
        ),
    )(blk, src, meta, ohf, ohb, ice, ocean, rates, land, masked)

    def flat(values):
        return values[:, :chans].transpose(1, 0, 2).reshape(cats, fields, cells)

    return flat(ice), flat(flux)


def solution(mesh):
    placed = (
        P(None, None, ("ice", "ocn")),
        P(None, None, ("ice", "ocn")),
        P(),
        P(("ice", "ocn"), None, None),
        P(("ice", "ocn"), None),
        P(("ice", "ocn"), None),
        P(("ice", "ocn")),
        P(("ice", "ocn")),
    )
    return jax.shard_map(
        on_device,
        mesh=mesh,
        in_specs=placed,
        out_specs=(P(None, None, ("ice", "ocn")), P(None, None, ("ice", "ocn"))),
        check_vma=False,
    )
```

```python
import functools

import jax
import jax.numpy as jnp
from jax import lax
from jax.experimental import pallas as pl
from jax.experimental.pallas import tpu as pltpu
from jax.sharding import PartitionSpec as P

CAP = 2
AXES = ("ice", "ocn")
LINE = 4
ROWS = 16


def spread(first, count):
    return sorted(range(first, count), key=lambda c: min(c, count - c))


def kernel(
    sizes, blk_ref, tile_ref, names_ref,
    ice_in, ocean_ref, rate_ref, land_ref, w_ref,
    ice_ref, flux_out,
    names_in, names, psend, prec, zsend, zrec, frec, bsend, ret, contrib, total,
    ns_s, ns_r, nl,
    ps_s, ps_r, zs_s, zs_r, fs_s, fs_r, bs_s, bs_r,
):
    Z, Y, N, tiles = sizes
    chans, width = ice_in.shape[1:]
    per = N * CAP
    steps = chans // ROWS
    ice_id, ocn_id = lax.axis_index("ice"), lax.axis_index("ocn")
    z, y = ocn_id // Y, ocn_id % Y
    p = ice_id * Y + y

    def plane(j):
        q = (p + j) % N
        return {"ice": q // Y, "ocn": z * Y + q % Y}

    def line(c):
        return {"ice": ice_id, "ocn": ((z + c) % Z) * Y + y}

    barrier = pltpu.get_barrier_semaphore()
    for j in range(1, N):
        pl.semaphore_signal(barrier, inc=1, device_id=plane(j), device_id_type=pl.DeviceIdType.MESH)
    for c in range(1, Z):
        pl.semaphore_signal(barrier, inc=1, device_id=line(c), device_id_type=pl.DeviceIdType.MESH)
    pl.semaphore_wait(barrier, N - 1 + Z - 1)

    def remote(src, dst, s, r, dev):
        return pltpu.make_async_remote_copy(
            src_ref=src, dst_ref=dst, send_sem=s, recv_sem=r,
            device_id=dev, device_id_type=pl.DeviceIdType.MESH,
        )

    def pcopy(c, j):
        at = pl.ds((c * N + j) * CAP, CAP)
        return remote(psend.at[at], prec.at[at], ps_s.at[c, j], ps_r.at[c, j], plane(j))

    def bcopy(c, j):
        at = pl.ds((c * N + j) * CAP, CAP)
        return remote(bsend.at[at], ret.at[at], bs_s.at[c, j], bs_r.at[c, j], plane(N - j))

    def zcopy(c):
        return remote(zsend.at[c], zrec.at[c], zs_s.at[c], zs_r.at[c], line(c))

    def fcopy(c):
        return remote(frec[0], frec[c], fs_s.at[c], fs_r.at[c], line(c))

    def ncopy(j):
        return remote(names_ref.at[j], names_in.at[j], ns_s.at[j], ns_r.at[j], plane(j))

    def nlocal(j):
        held = names_in if j else names_ref
        return pltpu.make_async_copy(held.at[j], names.at[j], nl.at[j])

    def name(c, n):
        return names[n // CAP, 0, c * CAP + n % CAP]

    for j in range(1, N):
        ncopy(j).start()
    nlocal(0).start()

    def gather(load, place, start, finish):
        def rows(r, carry):
            at = pl.ds(pl.multiple_of(r * ROWS, ROWS), ROWS)

            def add(k, accs):
                x = load(k, at)
                to = jnp.full((ROWS, width), place(k), jnp.int32)
                return tuple(accs[t] + jnp.where(to == t, x, 0.0) for t in range(tiles))

            accs = lax.fori_loop(0, per, add, tuple(start(t, at) for t in range(tiles)), unroll=True)
            for t in range(tiles):
                finish(t, at, accs[t])
            return carry

        lax.fori_loop(0, steps, rows, 0)

    ice_ref[...] = ice_in[...]
    near = spread(1, Z)
    for j in range(1, N):
        ncopy(j).wait_recv()
        nlocal(j).start()
    for j in range(N):
        nlocal(j).wait()

    def turn(number, carry):
        for c in near[::-1] + [0]:
            for n in range(per):
                slot = c * per + n
                block = blk_ref[slot]
                prod = jnp.dot(
                    ice_ref[tile_ref[slot] % tiles], w_ref[block], preferred_element_type=jnp.float32
                ).astype(jnp.bfloat16)
                if n < CAP:
                    prec[slot] = prod
                else:
                    psend[slot] = prod
            for j in range(1, N):
                pcopy(c, j).start()
        for c in near[::-1] + [0]:
            for j in range(1, N):
                pcopy(c, j).wait_recv()
            base = c * per

            def load(k, at):
                return prec[base + k, at, :].astype(jnp.float32)

            def start(t, at):
                return jnp.zeros((ROWS, width), jnp.float32)

            def finish(t, at, acc):
                if c == 0:
                    total[t, at, :] = acc
                else:
                    zsend[c, t, at, :] = acc.astype(jnp.bfloat16)

            gather(load, lambda k: name(c, k), start, finish)
            if c:
                zcopy(c).start()
        for c in near:
            zcopy(c).wait_recv()

        def flux_rows(r, carry):
            at = pl.ds(pl.multiple_of(r * ROWS, ROWS), ROWS)
            for t in range(tiles):
                acc = total[t, at, :]
                for c in near:
                    acc = acc + zrec[c, t, at, :].astype(jnp.float32)
                acc = jnp.tanh(acc + ocean_ref[t, at, :].astype(jnp.float32))
                frec[0][t, at, :] = acc.astype(jnp.bfloat16)
                total[t, at, :] = jnp.zeros((ROWS, width), jnp.float32)
            return carry

        lax.fori_loop(0, steps, flux_rows, 0)
        for c in near:
            fcopy(c).start()
        for c in [0] + near:
            held = (Z - c) % Z
            if c:
                fcopy(held).wait_recv()
            for n in range(per):
                slot = c * per + n
                tile = frec[held][name(c, n) % tiles]
                if n < CAP:
                    ret[slot] = tile
                else:
                    bsend[slot] = tile
            for j in range(1, N):
                bcopy(c, j).start()
        for c in [0] + near:
            for j in range(1, N):
                bcopy(c, j).wait_recv()
            base = c * per
            for n in range(per):
                contrib[n] = lax.dot_general(
                    ret[base + n], w_ref[blk_ref[base + n]], (((1,), (1,)), ((), ())),
                    preferred_element_type=jnp.float32,
                )

            def load(k, at):
                return contrib[k, at, :]

            def start(t, at):
                return total[t, at, :]

            def finish(t, at, acc):
                total[t, at, :] = acc

            gather(load, lambda k: tile_ref[base + k], start, finish)

        def ice_rows(r, carry):
            at = pl.ds(pl.multiple_of(r * ROWS, ROWS), ROWS)
            rate = rate_ref[at, :]
            for t in range(tiles):
                old = ice_ref[t, at, :].astype(jnp.float32)
                new = land_ref[pl.ds(t, 1), :] * (old + rate * jnp.tanh(total[t, at, :]))
                ice_ref[t, at, :] = new.astype(jnp.bfloat16)
            return carry

        lax.fori_loop(0, steps, ice_rows, 0)
        for c in range(Z):
            for j in range(1, N):
                pcopy(c, j).wait_send()
                bcopy(c, j).wait_send()
        for c in near:
            zcopy(c).wait_send()
            fcopy(c).wait_send()
        return carry

    lax.fori_loop(0, 2, turn, 0)
    flux_out[...] = frec[0][...]
    for j in range(1, N):
        ncopy(j).wait_send()


def on_device(
    ice_state, ocean_state, ice_rate, block_weights, block_route, block_tiles, block_valid, ice_mask
):
    cats, fields, cells = ice_state.shape
    chans = cats * fields
    rows = -(-chans // ROWS) * ROWS
    blocks, width, unused = block_weights.shape
    tiles = cells // width
    outer = lax.axis_size("ocn")
    Z = LINE if outer % LINE == 0 else outer
    Y = outer // Z
    N = lax.axis_size("ice") * Y
    ice_id, ocn_id = lax.axis_index("ice"), lax.axis_index("ocn")
    z, y = ocn_id // Y, ocn_id % Y
    p = ice_id * Y + y

    def number(q, zz):
        return ((q // Y) * outer + zz * Y + q % Y).astype(jnp.int32)

    route = block_route[:, 0]
    source, target = block_tiles[:, 0], block_tiles[:, 1]
    order = jnp.arange(blocks, dtype=jnp.int32)
    earlier = (route[None, :] == route[:, None]) & (order[None, :] < order[:, None])
    slot = jnp.sum(earlier.astype(jnp.int32), axis=1)
    js = jnp.arange(N, dtype=jnp.int32)
    cs = jnp.arange(Z, dtype=jnp.int32)
    ks = jnp.arange(CAP, dtype=jnp.int32)
    dest = number((p + js)[None, :] % N, ((z + cs) % Z)[:, None])
    code = route * CAP + slot
    sel = code == (dest[:, :, None] * CAP + ks)[..., None]
    blk = jnp.sum(jnp.where(sel, order, 0), axis=-1).reshape(-1)
    src = tiles + jnp.sum(jnp.where(sel, source - tiles, 0), axis=-1).reshape(-1)
    names = tiles + jnp.sum(jnp.where(sel, target - tiles, 0), axis=-1)
    names = names.transpose(1, 0, 2).reshape(N, 1, Z * CAP)
    names = jnp.pad(names, ((0, 0), (0, 0), (0, width - Z * CAP)))
    live = jnp.arange(width, dtype=jnp.int32)[None, :] < block_valid[:, None]
    masked = jnp.where(live[:, :, None], block_weights, jnp.zeros((), jnp.bfloat16))

    def tiled(values):
        values = values.reshape(chans, tiles, width).transpose(1, 0, 2)
        return jnp.pad(values, ((0, 0), (0, rows - chans), (0, 0)))

    ice = tiled(ice_state * ice_mask.astype(jnp.bfloat16)[None, None, :])
    ocean = tiled(ocean_state)
    rates = jnp.broadcast_to(jnp.pad(ice_rate.reshape(chans, 1), ((0, rows - chans), (0, 0))), (rows, width))
    land = ice_mask.astype(jnp.float32).reshape(tiles, width)
    slots = Z * N * CAP
    smem, vmem = pl.BlockSpec(memory_space=pltpu.SMEM), pl.BlockSpec(memory_space=pltpu.VMEM)
    tile = (rows, width)
    ice, flux = pl.pallas_call(
        functools.partial(kernel, (Z, Y, N, tiles)),
        out_shape=(jax.ShapeDtypeStruct((tiles,) + tile, jnp.bfloat16),) * 2,
        in_specs=[smem] * 2 + [vmem] * 6,
        out_specs=(vmem, vmem),
        scratch_shapes=[
            pltpu.VMEM((N, 1, width), jnp.int32),
            pltpu.SMEM((N, 1, width), jnp.int32),
            pltpu.VMEM((slots,) + tile, jnp.bfloat16),
            pltpu.VMEM((slots,) + tile, jnp.bfloat16),
            pltpu.VMEM((Z, tiles) + tile, jnp.bfloat16),
            pltpu.VMEM((Z, tiles) + tile, jnp.bfloat16),
            tuple(pltpu.VMEM((tiles,) + tile, jnp.bfloat16) for c in range(Z)),
            pltpu.VMEM((slots,) + tile, jnp.bfloat16),
            pltpu.VMEM((slots,) + tile, jnp.bfloat16),
            pltpu.VMEM((N * CAP,) + tile, jnp.float32),
            pltpu.VMEM((tiles,) + tile, jnp.float32),
            pltpu.SemaphoreType.DMA((N,)),
            pltpu.SemaphoreType.DMA((N,)),
            pltpu.SemaphoreType.DMA((N,)),
            pltpu.SemaphoreType.DMA((Z, N)),
            pltpu.SemaphoreType.DMA((Z, N)),
            pltpu.SemaphoreType.DMA((Z,)),
            pltpu.SemaphoreType.DMA((Z,)),
            pltpu.SemaphoreType.DMA((Z,)),
            pltpu.SemaphoreType.DMA((Z,)),
            pltpu.SemaphoreType.DMA((Z, N)),
            pltpu.SemaphoreType.DMA((Z, N)),
        ],
        compiler_params=pltpu.CompilerParams(
            collective_id=0, has_side_effects=True, vmem_limit_bytes=60 * 1024 * 1024
        ),
    )(blk, src, names, ice, ocean, rates, land, masked)

    def flat(values):
        return values[:, :chans].transpose(1, 0, 2).reshape(cats, fields, cells)

    return flat(ice), flat(flux)


def solution(mesh):
    placed = (
        P(None, None, ("ice", "ocn")),
        P(None, None, ("ice", "ocn")),
        P(),
        P(("ice", "ocn"), None, None),
        P(("ice", "ocn"), None),
        P(("ice", "ocn"), None),
        P(("ice", "ocn")),
        P(("ice", "ocn")),
    )
    return jax.shard_map(
        on_device,
        mesh=mesh,
        in_specs=placed,
        out_specs=(P(None, None, ("ice", "ocn")), P(None, None, ("ice", "ocn"))),
        check_vma=False,
    )
```
